32 devices in a mesh: dp: 2 (over x), col: 4 (over z), row: 4 (over y, core).
Axes of the slice: x: 2, y: 2, z: 4, core: 2. Of those that a mesh axis runs over, the one named last changes fastest.
Arguments:
- x_in: bfloat16 [8, 768, 2048], P(('dp', 'row'), None, 'col'), parts along dimension 0
- ln1_scale: float32 [2048], P('col')
- ln1_shift: float32 [2048], P('col')
- w_qkv: bfloat16 [2048, 6144], P('row', 'col')
- b_qkv: float32 [32, 192], P('col')
- w_o: bfloat16 [2048, 2048], P('row', 'col')
- b_o: float32 [2048], P('col')
- ln2_scale: float32 [2048], P('col')
- ln2_shift: float32 [2048], P('col')
- w_in: bfloat16 [2048, 8192], P('row', 'col')
- b_in: float32 [8192], P('col')
- w_out: bfloat16 [8192, 2048], P('row', 'col')
- b_out: float32 [2048], P('col')
- grad_out: bfloat16 [8, 768, 2048], P(('dp', 'row'), None, 'col'), parts along dimension 0
Outputs:
- output 1: bfloat16 [8, 768, 2048], P(('dp', 'row'), None, 'col'), parts along dimension 0
- output 2: bfloat16 [8, 768, 2048], P(('dp', 'row'), None, 'col'), parts along dimension 0
- output 3: float32 [4096], P(('dp', 'col')), parts along dimension 0
- output 4: float32 [4096], P(('dp', 'col')), parts along dimension 0
- output 5: bfloat16 [4096, 6144], P(('dp', 'row'), 'col'), parts along dimension 0
- output 6: float32 [64, 192], P(('dp', 'col')), parts along dimension 0
- output 7: bfloat16 [4096, 2048], P(('dp', 'row'), 'col'), parts along dimension 0
- output 8: float32 [4096], P(('dp', 'col')), parts along dimension 0
- output 9: float32 [4096], P(('dp', 'col')), parts along dimension 0
- output 10: float32 [4096], P(('dp', 'col')), parts along dimension 0
- output 11: bfloat16 [4096, 8192], P(('dp', 'row'), 'col'), parts along dimension 0
- output 12: float32 [16384], P(('dp', 'col')), parts along dimension 0
- output 13: bfloat16 [16384, 2048], P(('dp', 'row'), 'col'), parts along dimension 0
- output 14: float32 [4096], P(('dp', 'col')), parts along dimension 0
There are 2 independent parts. The reference program is written for one: setup_inputs(seed, part) draws one part's arguments, and reference() takes and returns one part's arrays. A program takes and returns all parts, laid end to end along the dimension named above; an argument that names none is the same for every part.
All inputs are finite; a program needn't handle non-finite values.
Results may differ from the reference program's by a relative error of at most 0.0113486.
Values are sent between devices in bfloat16 or wider.
A program may use at most 1 GiB of HBM per device.

```python
import jax
import jax.numpy as jnp
from jax import lax

BATCH = 4
SEQ_LEN = 768
D_MODEL = 2048
NUM_HEADS = 32
HEAD_DIM = 64
D_FF = 8192
LN_EPS = 1e-5


def setup_inputs(seed: int = 0, part: int = 0) -> dict:
    shared = jax.random.split(jax.random.key(seed), 12)
    part_keys = jax.random.split(jax.random.fold_in(jax.random.key(seed + 1), part), 3)

    def draw_normal(key_in, arr_shape, spread):
        return jax.random.normal(key_in, arr_shape, jnp.float32) * spread

    act_shape = (BATCH, SEQ_LEN, D_MODEL)
    feat_mean = draw_normal(part_keys[0], (D_MODEL,), 1.0)
    x_in = (draw_normal(part_keys[1], act_shape, 1.0) + feat_mean).astype(jnp.bfloat16)
    return {
        'x_in': x_in,
        'ln1_scale': 1.0 + draw_normal(shared[0], (D_MODEL,), 0.3),
        'ln1_shift': draw_normal(shared[1], (D_MODEL,), 0.3),
        'w_qkv': draw_normal(shared[2], (D_MODEL, 3 * D_MODEL), D_MODEL ** -0.5).astype(jnp.bfloat16),
        'b_qkv': draw_normal(shared[3], (NUM_HEADS, 3 * HEAD_DIM), 0.5),
        'w_o': draw_normal(shared[4], (D_MODEL, D_MODEL), D_MODEL ** -0.5).astype(jnp.bfloat16),
        'b_o': draw_normal(shared[5], (D_MODEL,), 0.5),
        'ln2_scale': 1.0 + draw_normal(shared[6], (D_MODEL,), 0.3),
        'ln2_shift': draw_normal(shared[7], (D_MODEL,), 0.3),
        'w_in': draw_normal(shared[8], (D_MODEL, D_FF), D_MODEL ** -0.5).astype(jnp.bfloat16),
        'b_in': draw_normal(shared[9], (D_FF,), 0.5),
        'w_out': draw_normal(shared[10], (D_FF, D_MODEL), D_FF ** -0.5).astype(jnp.bfloat16),
        'b_out': draw_normal(shared[11], (D_MODEL,), 0.5),
        'grad_out': draw_normal(part_keys[2], act_shape, 1.0).astype(jnp.bfloat16),
    }


def layer_norm(act_in, ln_scale, ln_shift):
    act_f32 = act_in.astype(jnp.float32)
    mean_val = jnp.mean(act_f32, axis=-1, keepdims=True)
    variance = jnp.mean(act_f32 * act_f32, axis=-1, keepdims=True) - mean_val * mean_val
    return ((act_f32 - mean_val) * lax.rsqrt(variance + LN_EPS) * ln_scale + ln_shift).astype(jnp.bfloat16)


def attend_one(head_item):
    scores = jnp.dot(head_item[0], head_item[1].T, preferred_element_type=jnp.float32) * HEAD_DIM ** -0.5
    query_pos = lax.broadcasted_iota(jnp.int32, (SEQ_LEN, SEQ_LEN), 0)
    key_pos = lax.broadcasted_iota(jnp.int32, (SEQ_LEN, SEQ_LEN), 1)
    attn_probs = jax.nn.softmax(jnp.where(key_pos <= query_pos, scores, -1e30), axis=-1)
    return jnp.dot(attn_probs.astype(jnp.bfloat16), head_item[2], preferred_element_type=jnp.float32).astype(jnp.bfloat16)


def layer_forward(x_in, ln1_scale, ln1_shift, w_qkv, b_qkv, w_o, b_o, ln2_scale, ln2_shift, w_in, b_in, w_out, b_out):
    tokens = BATCH * SEQ_LEN
    x_rows = x_in.reshape(tokens, D_MODEL)
    normed1 = layer_norm(x_rows, ln1_scale, ln1_shift)
    qkv_rows = (jnp.dot(normed1, w_qkv, preferred_element_type=jnp.float32) + b_qkv.reshape(3 * D_MODEL)).astype(jnp.bfloat16)
    head_items = qkv_rows.reshape(BATCH, SEQ_LEN, NUM_HEADS, 3, HEAD_DIM).transpose(0, 2, 3, 1, 4)
    head_items = head_items.reshape(BATCH * NUM_HEADS, 3, SEQ_LEN, HEAD_DIM)
    attn_items = lax.map(jax.checkpoint(attend_one), head_items)
    attn_rows = attn_items.reshape(BATCH, NUM_HEADS, SEQ_LEN, HEAD_DIM).transpose(0, 2, 1, 3).reshape(tokens, D_MODEL)
    resid_rows = (x_rows.astype(jnp.float32) + jnp.dot(attn_rows, w_o, preferred_element_type=jnp.float32) + b_o).astype(jnp.bfloat16)
    normed2 = layer_norm(resid_rows, ln2_scale, ln2_shift)
    pre_act = jnp.dot(normed2, w_in, preferred_element_type=jnp.float32) + b_in
    hidden = jax.nn.gelu(pre_act, approximate=True).astype(jnp.bfloat16)
    out_rows = (resid_rows.astype(jnp.float32) + jnp.dot(hidden, w_out, preferred_element_type=jnp.float32) + b_out).astype(jnp.bfloat16)
    return out_rows.reshape(BATCH, SEQ_LEN, D_MODEL)


def reference(x_in, ln1_scale, ln1_shift, w_qkv, b_qkv, w_o, b_o, ln2_scale, ln2_shift, w_in, b_in, w_out, b_out, grad_out):
    out_val, pullback = jax.vjp(layer_forward, x_in, ln1_scale, ln1_shift, w_qkv, b_qkv, w_o, b_o, ln2_scale, ln2_shift, w_in, b_in, w_out, b_out)
    grads = pullback(grad_out)
    return (out_val, grads[0], grads[1], grads[2], grads[3], grads[4], grads[5], grads[6], grads[7], grads[8], grads[9], grads[10], grads[11], grads[12])
```

```python
import jax
import jax.numpy as jnp
from jax import lax
from jax.sharding import PartitionSpec as P

LN_EPS = 1e-5
BF16 = jnp.bfloat16
F32 = jnp.float32


def gelu_tanh(pre_act):
    return jax.nn.gelu(pre_act, approximate=True)


def attend_one(query_rows, key_rows, value_rows):
    seq_len, head_dim = query_rows.shape
    scores = lax.dot_general(query_rows, key_rows, (((1,), (1,)), ((), ())), preferred_element_type=jnp.float32)
    query_pos = lax.broadcasted_iota(jnp.int32, (seq_len, 1), 0)
    key_pos = lax.broadcasted_iota(jnp.int32, (1, seq_len), 1)
    attn_probs = jax.nn.softmax(jnp.where(key_pos <= query_pos, scores * head_dim ** -0.5, -1e30), axis=-1)
    return jnp.dot(attn_probs.astype(jnp.bfloat16), value_rows, preferred_element_type=jnp.float32).astype(jnp.bfloat16)


def attend_item(head_item):
    return attend_one(head_item[0], head_item[1], head_item[2])


def attend_item_back(item_pair):
    head_item, grad_item = item_pair
    pullback = jax.vjp(attend_one, head_item[0], head_item[1], head_item[2])[1]
    return jnp.stack(pullback(grad_item))


def dot_nn(lhs, rhs):
    return jnp.dot(lhs, rhs, preferred_element_type=F32)


def dot_nt(lhs, rhs):
    return lax.dot_general(lhs, rhs, (((1,), (1,)), ((), ())), preferred_element_type=F32)


def dot_tn(lhs, rhs):
    return lax.dot_general(lhs, rhs, (((0,), (0,)), ((), ())), preferred_element_type=F32)


def norm_stats(act_f32, width):
    mean_val = jnp.sum(act_f32, axis=-1, keepdims=True) / width
    mean_sq = jnp.sum(act_f32 * act_f32, axis=-1, keepdims=True) / width
    return mean_val, lax.rsqrt(mean_sq - mean_val * mean_val + LN_EPS)


def solution(mesh):
    n_row, n_col = mesh.shape['row'], mesh.shape['col']
    act_spec = P(('dp', 'row'), None, 'col')
    vec_spec = P('col')
    mat_spec = P('row', 'col')
    head_spec = P('col', None)
    gvec_spec = P(('dp', 'col'))
    gmat_spec = P(('dp', 'row'), 'col')
    ghead_spec = P(('dp', 'col'), None)

    def flip_row(val, bits):
        return lax.ppermute(val, 'row', [(src, src ^ bits) for src in range(n_row)])

    def shift_col(val, step):
        return lax.ppermute(val, 'col', [(src, (src + step) % n_col) for src in range(n_col)])

    def swap_axes(val):
        pairs = [(r * n_col + c, c * n_col + r) for r in range(n_row) for c in range(n_col)]
        return lax.ppermute(val, ('col', 'row'), pairs)

    def gather_row(w_blk, axis):
        row = lax.axis_index('row')
        far = flip_row(w_blk, 2)
        mate = flip_row(w_blk, 1)
        far_mate = flip_row(far, 1)
        size = w_blk.shape[axis]
        shape = list(w_blk.shape)
        shape[axis] = n_row * size
        full = jnp.zeros(shape, w_blk.dtype)
        for bits, part in ((0, w_blk), (1, mate), (2, far), (3, far_mate)):
            full = lax.dynamic_update_slice_in_dim(full, part, (row ^ bits) * size, axis)
        return full

    def scatter_row(make_part):
        row = lax.axis_index('row')
        sent_a, sent_b = make_part(row ^ 3), make_part(row ^ 1)
        got_a, got_b = flip_row(sent_a, 1), flip_row(sent_b, 1)
        far = flip_row(make_part(row ^ 2) + got_a, 2)
        return (make_part(row) + got_b + far).astype(BF16)

    def sum_row(val):
        val = val + flip_row(val, 1)
        return val + flip_row(val, 2)

    def layer_block(x_blk, ln1_scale, ln1_shift, w_qkv, b_qkv, w_o, b_o, ln2_scale, ln2_shift, w_in, b_in, w_out, b_out, grad_blk):
        seq_count, seq_len, d_local = x_blk.shape
        tokens = seq_count * seq_len
        heads_local, qkv_width = b_qkv.shape
        head_dim = qkv_width // 3
        width = d_local * n_col
        col = lax.axis_index('col')
        x_rows = x_blk.reshape(tokens, d_local)
        grad_rows = grad_blk.reshape(tokens, d_local)

        def col_block(val, axis, index, size):
            return lax.dynamic_slice_in_dim(val, index * size, size, axis)

        vecs = lax.all_gather(jnp.stack([ln1_scale, ln1_shift, b_o, ln2_scale, ln2_shift]), 'col', axis=1, tiled=True)
        s1, t1, bo, s2, t2 = [vecs[i:i + 1] for i in range(5)]

        x_full = lax.all_gather(x_rows, 'col', axis=1, tiled=True)
        wq = gather_row(w_qkv, 0)
        x32 = x_full.astype(F32)
        mean1, inv1 = norm_stats(x32, width)
        h1 = ((x32 - mean1) * inv1 * s1 + t1).astype(BF16)
        qkv_rows = (dot_nn(h1, wq) + b_qkv.reshape(heads_local * qkv_width)).astype(BF16)
        head_items = qkv_rows.reshape(seq_count, seq_len, heads_local, 3, head_dim).transpose(0, 2, 3, 1, 4).reshape(seq_count * heads_local, 3, seq_len, head_dim)
        attn_items = lax.map(attend_item, head_items)
        attn_rows = attn_items.reshape(seq_count, heads_local, seq_len, head_dim).transpose(0, 2, 1, 3).reshape(tokens, d_local)
        attn_full = lax.all_gather(attn_rows, 'col', axis=1, tiled=True)

        wo = gather_row(lax.all_gather(w_o, 'col', axis=1, tiled=True), 0)
        wi = gather_row(w_in, 0)
        wt = gather_row(swap_axes(w_out), 1)
        g_full = lax.all_gather(grad_rows, 'col', axis=1, tiled=True)

        r1 = (x32 + dot_nn(attn_full, wo) + bo).astype(BF16)
        r32 = r1.astype(F32)
        mean2, inv2 = norm_stats(r32, width)
        h2 = ((r32 - mean2) * inv2 * s2 + t2).astype(BF16)
        pre_act = dot_nn(h2, wi) + b_in
        hidden, gelu_back = jax.vjp(gelu_tanh, pre_act)
        hidden = hidden.astype(BF16)

        grad_hidden = dot_nt(g_full, wt).astype(BF16)
        grad_pre = gelu_back(grad_hidden.astype(F32))[0].astype(BF16)
        tok_local = tokens // n_col
        gn2 = lax.psum_scatter(dot_nt(grad_pre, wi), 'col', scatter_dimension=0, tiled=True).astype(BF16).astype(F32)
        r_tok = col_block(r1, 0, col, tok_local).astype(F32)
        mean_t, inv_t = col_block(mean2, 0, col, tok_local), col_block(inv2, 0, col, tok_local)
        hat_t = (r_tok - mean_t) * inv_t
        gs2 = jnp.stack([jnp.sum(gn2 * hat_t, axis=0), jnp.sum(gn2, axis=0)])
        ghat = gn2 * s2
        gin = inv_t * (ghat - jnp.mean(ghat, axis=-1, keepdims=True) - hat_t * jnp.mean(ghat * hat_t, axis=-1, keepdims=True))
        gr_tok = (col_block(g_full, 0, col, tok_local).astype(F32) + gin).astype(BF16)
        gr = lax.all_gather(gr_tok, 'col', axis=0, tiled=True)
        gr_mine = col_block(gr, 1, col, d_local)

        grad_attn = dot_nt(gr, col_block(wo, 0, col, d_local)).astype(BF16)
        grad_items = grad_attn.reshape(seq_count, seq_len, heads_local, head_dim).transpose(0, 2, 1, 3).reshape(seq_count * heads_local, seq_len, head_dim)
        grad_heads = lax.map(attend_item_back, (head_items, grad_items))
        grad_qkv = grad_heads.reshape(seq_count, heads_local, 3, seq_len, head_dim).transpose(0, 3, 1, 2, 4).reshape(tokens, heads_local * qkv_width)

        hidden_late, _ = lax.optimization_barrier((hidden, gr))
        out_part = lax.psum_scatter(dot_nn(hidden_late, wt), 'col', scatter_dimension=1, tiled=True)
        out_rows = (col_block(r1, 1, col, d_local).astype(F32) + out_part + b_out).astype(BF16)

        gn1 = lax.psum_scatter(dot_nt(grad_qkv, wq), 'col', scatter_dimension=1, tiled=True).astype(BF16).astype(F32)
        hat1 = (x_rows.astype(F32) - mean1) * inv1
        ghat1 = gn1 * ln1_scale
        sums = jnp.stack([jnp.sum(ghat1, axis=-1), jnp.sum(ghat1 * hat1, axis=-1)])
        sums = (sums + shift_col(sums, 1) + shift_col(sums, 2) + shift_col(sums, 3)) / width
        gx = gr_mine.astype(F32) + inv1 * (ghat1 - sums[0][:, None] - hat1 * sums[1][:, None])
        grad_x = gx.astype(BF16)

        grad_wout = swap_axes(scatter_row(lambda j: dot_tn(hidden, col_block(g_full, 1, j, d_local))))
        grad_win = scatter_row(lambda j: dot_tn(col_block(h2, 1, j, width // n_row), grad_pre))
        grad_wo = scatter_row(lambda j: dot_tn(col_block(attn_full, 1, j, width // n_row), gr_mine))
        grad_wqkv = scatter_row(lambda j: dot_tn(col_block(h1, 1, j, width // n_row), grad_qkv))

        def tok_sum(val):
            return jnp.sum(val.astype(F32), axis=0)

        ln2_part = col_block(gs2, 1, col, d_local)
        for step in range(1, n_col):
            ln2_part = ln2_part + shift_col(col_block(gs2, 1, (col + step) % n_col, d_local), step)
        early = sum_row(jnp.concatenate([ln2_part.reshape(-1), tok_sum(grad_rows), tok_sum(gr_mine), tok_sum(grad_pre)]))
        gl2s, gl2t, gbout, gbo, gbin = jnp.split(early, [d_local * k for k in range(1, 5)])
        gbqkv = sum_row(tok_sum(grad_qkv))
        late = sum_row(jnp.stack([jnp.sum(gn1 * hat1, axis=0), jnp.sum(gn1, axis=0)]))
        return (out_rows.reshape(x_blk.shape), grad_x.reshape(x_blk.shape), late[0], late[1], grad_wqkv, gbqkv.reshape(heads_local, qkv_width), grad_wo, gbo, gl2s, gl2t, grad_win, gbin, grad_wout, gbout)

    return jax.shard_map(layer_block, mesh=mesh,
                         in_specs=(act_spec, vec_spec, vec_spec, mat_spec, head_spec, mat_spec, vec_spec, vec_spec, vec_spec, mat_spec, vec_spec, mat_spec, vec_spec, act_spec),
                         out_specs=(act_spec, act_spec, gvec_spec, gvec_spec, gmat_spec, ghead_spec, gmat_spec, gvec_spec, gvec_spec, gvec_spec, gmat_spec, gvec_spec, gmat_spec, gvec_spec),
                         check_vma=False)
```

```python
import functools

import jax
import jax.numpy as jnp
from jax import lax
from jax.experimental import pallas as pl
from jax.experimental.pallas import tpu as pltpu
from jax.sharding import PartitionSpec as P


LN_EPS = 1e-5
BF16 = jnp.bfloat16
F32 = jnp.float32
LOG2E = 1.4426950408889634
MASKED = -1e30


def gelu_tanh(pre_act):
    return jax.nn.gelu(pre_act, approximate=True)


def dot_nn(lhs, rhs):
    return jnp.dot(lhs, rhs, preferred_element_type=F32)


def dot_nt(lhs, rhs):
    return lax.dot_general(lhs, rhs, (((1,), (1,)), ((), ())), preferred_element_type=F32)


def dot_tn(lhs, rhs):
    return lax.dot_general(lhs, rhs, (((0,), (0,)), ((), ())), preferred_element_type=F32)


def split_heads(blk, base, size):
    return blk[:, base:base + size], blk[:, base + size:base + 2 * size], blk[:, base + 2 * size:base + 3 * size]


def causal_mask(step):
    key_pos = lax.broadcasted_iota(jnp.int32, (step, step), 0)
    return key_pos <= lax.broadcasted_iota(jnp.int32, (step, step), 1)


def attn_fwd_kernel(head_dim, step, qkv_ref, out_ref, stat_ref):
    blocks = qkv_ref.shape[0] // step
    factor = head_dim ** -0.5 * LOG2E
    mask = causal_mask(step)
    blk = qkv_ref[...]
    for i in range(blocks):
        rows = slice(i * step, (i + 1) * step)
        outs = []
        for j in range(2):
            query, key, value = split_heads(blk, j * 3 * head_dim, head_dim)
            scores = [dot_nt(key[b * step:(b + 1) * step], query[rows]) for b in range(i + 1)]
            scores[i] = jnp.where(mask, scores[i], MASKED)
            top = functools.reduce(jnp.maximum, [jnp.max(s, axis=0, keepdims=True) for s in scores])
            exps = [jnp.exp2((s - top) * factor) for s in scores]
            inv = 1.0 / sum(jnp.sum(e, axis=0, keepdims=True) for e in exps)
            outs.append(sum(dot_tn(value[b * step:(b + 1) * step], (e * inv).astype(BF16)) for b, e in enumerate(exps)))
            stat_ref[0, 2 * j:2 * j + 1, rows] = top
            stat_ref[0, 2 * j + 1:2 * j + 2, rows] = inv
        out_ref[rows, :] = jnp.concatenate(outs, axis=0).T.astype(BF16)


def attn_bwd_kernel(head_dim, step, qkv_ref, grad_ref, stat_ref, out_ref):
    blocks = qkv_ref.shape[0] // step
    scale = head_dim ** -0.5
    factor = scale * LOG2E
    mask = causal_mask(step)
    blk = qkv_ref[...]
    for j in range(2):
        base = j * 3 * head_dim
        query, key, value = split_heads(blk, base, head_dim)
        grad = grad_ref[:, j * head_dim:(j + 1) * head_dim]
        grad_key, grad_value = [0.0] * blocks, [0.0] * blocks
        for i in range(blocks):
            rows = slice(i * step, (i + 1) * step)
            top = stat_ref[0, 2 * j:2 * j + 1, rows]
            inv = stat_ref[0, 2 * j + 1:2 * j + 2, rows]
            probs, grads, dots = [], [], 0.0
            for b in range(i + 1):
                keys = slice(b * step, (b + 1) * step)
                scores = dot_nt(key[keys], query[rows])
                if b == i:
                    scores = jnp.where(mask, scores, MASKED)
                prob = jnp.exp2((scores - top) * factor) * inv
                grad_prob = dot_nt(value[keys], grad[rows])
                dots = dots + jnp.sum(prob * grad_prob, axis=0, keepdims=True)
                probs.append(prob)
                grads.append(grad_prob)
            grad_query = 0.0
            for b in range(i + 1):
                keys = slice(b * step, (b + 1) * step)
                grad_score = (probs[b] * (grads[b] - dots)).astype(BF16)
                grad_value[b] = grad_value[b] + dot_nn(probs[b].astype(BF16), grad[rows])
                grad_key[b] = grad_key[b] + dot_nn(grad_score, query[rows])
                grad_query = grad_query + dot_tn(key[keys], grad_score)
            out_ref[rows, base:base + head_dim] = (grad_query.T * scale).astype(BF16)
        for b in range(blocks):
            rows = slice(b * step, (b + 1) * step)
            out_ref[rows, base + head_dim:base + 2 * head_dim] = (grad_key[b] * scale).astype(BF16)
            out_ref[rows, base + 2 * head_dim:base + 3 * head_dim] = grad_value[b].astype(BF16)


def attn_cost(tokens, heads, head_dim, dots):
    return pl.CostEstimate(flops=dots * tokens * tokens * heads * head_dim, bytes_accessed=12 * tokens * heads * head_dim, transcendentals=tokens * tokens * heads // 2)


def attn_forward(qkv_rows, head_dim):
    tokens, width = qkv_rows.shape
    pairs = width // (6 * head_dim)
    return pl.pallas_call(
        functools.partial(attn_fwd_kernel, head_dim, 256),
        grid=(pairs,),
        in_specs=[pl.BlockSpec((tokens, 6 * head_dim), lambda p: (0, p))],
        out_specs=[pl.BlockSpec((tokens, 2 * head_dim), lambda p: (0, p)), pl.BlockSpec((1, 8, tokens), lambda p: (p, 0, 0))],
        out_shape=[jax.ShapeDtypeStruct((tokens, 2 * head_dim * pairs), BF16), jax.ShapeDtypeStruct((pairs, 8, tokens), F32)],
        cost_estimate=attn_cost(tokens, 2 * pairs, head_dim, 4),
        name="attn_fwd",
    )(qkv_rows)


def attn_backward(qkv_rows, grad_rows, stats, head_dim):
    tokens, width = qkv_rows.shape
    pairs = width // (6 * head_dim)
    return pl.pallas_call(
        functools.partial(attn_bwd_kernel, head_dim, 256),
        grid=(pairs,),
        in_specs=[pl.BlockSpec((tokens, 6 * head_dim), lambda p: (0, p)), pl.BlockSpec((tokens, 2 * head_dim), lambda p: (0, p)), pl.BlockSpec((1, 8, tokens), lambda p: (p, 0, 0))],
        out_specs=pl.BlockSpec((tokens, 6 * head_dim), lambda p: (0, p)),
        out_shape=jax.ShapeDtypeStruct((tokens, width), BF16),
        cost_estimate=attn_cost(tokens, 2 * pairs, head_dim, 10),
        name="attn_bwd",
    )(qkv_rows, grad_rows, stats)


def place_kernel(count, index_ref, *refs):
    for part in range(count):
        @pl.when(pl.program_id(0) == part)
        def _():
            refs[count][...] = refs[part][0]


def place_blocks(parts, where, shape, tile):
    count = len(parts)
    depth, rows, cols = parts[0].shape
    steps = rows // tile

    def part_map(own):
        def index_map(part, level, step, index_ref):
            active, past = part == own, part > own
            last = jnp.where(past, 1, 0)
            return jnp.where(active, level, last * (depth - 1)), jnp.where(active, step, last * (steps - 1)), 0

        return index_map

    def out_map(part, level, step, index_ref):
        slot = 2 * (part * depth + level)
        return index_ref[slot] * steps + step, index_ref[slot + 1]

    return pl.pallas_call(
        functools.partial(place_kernel, count),
        grid_spec=pltpu.PrefetchScalarGridSpec(
            num_scalar_prefetch=1,
            grid=(count, depth, steps),
            in_specs=[pl.BlockSpec((1, tile, cols), part_map(own)) for own in range(count)],
            out_specs=pl.BlockSpec((tile, cols), out_map),
        ),
        out_shape=jax.ShapeDtypeStruct(shape, parts[0].dtype),
        cost_estimate=pl.CostEstimate(flops=40000000, bytes_accessed=4 * shape[0] * shape[1], transcendentals=0),
        name="place_blocks",
    )(jnp.stack(where).astype(jnp.int32), *parts)


def norm_stats(act_f32, width):
    mean_val = jnp.sum(act_f32, axis=-1, keepdims=True) / width
    mean_sq = jnp.sum(act_f32 * act_f32, axis=-1, keepdims=True) / width
    return mean_val, lax.rsqrt(mean_sq - mean_val * mean_val + LN_EPS)


def solution(mesh):
    n_row, n_col = mesh.shape['row'], mesh.shape['col']
    act_spec = P(('dp', 'row'), None, 'col')
    vec_spec = P('col')
    mat_spec = P('row', 'col')
    head_spec = P('col', None)
    gvec_spec = P(('dp', 'col'))
    gmat_spec = P(('dp', 'row'), 'col')
    ghead_spec = P(('dp', 'col'), None)

    def flip_row(val, bits):
        return lax.ppermute(val, 'row', [(src, src ^ bits) for src in range(n_row)])

    def shift_col(val, step):
        return lax.ppermute(val, 'col', [(src, (src + step) % n_col) for src in range(n_col)])

    def cross(val, route):
        pairs = []
        for r in range(n_row):
            for c in range(n_col):
                row_to, col_to = route(r, c)
                if (row_to, col_to) != (r, c):
                    pairs.append((c * n_row + r, col_to * n_row + row_to))
        return lax.ppermute(val, ('col', 'row'), pairs)

    def cross_even(val):
        moved = cross(val, lambda r, c: (c, r))
        return jnp.where(lax.axis_index('row') == lax.axis_index('col'), val, moved)

    def pick(first, lead, other):
        return jnp.where(first, lead, other), jnp.where(first, other, lead)

    def tie(val, *others):
        return lax.optimization_barrier((val,) + others)[0]

    def swap_dp(val):
        return lax.ppermute(val, 'dp', [(0, 1), (1, 0)])

    def join_dp(half, axis):
        other = swap_dp(half)
        lead = lax.axis_index('dp') == 0
        return jnp.concatenate([jnp.where(lead, half, other), jnp.where(lead, other, half)], axis=axis)

    def half_dp(val, axis):
        size = val.shape[axis] // 2
        return lax.dynamic_slice_in_dim(val, lax.axis_index('dp') * size, size, axis)

    def gather_row(w_blk, far):
        row = lax.axis_index('row')
        mate = flip_row(w_blk, 1)
        far_mate = flip_row(far, 1)
        parts = [part[None] for part in (w_blk, mate, far, far_mate)]
        where = [coord for bits in range(4) for coord in (row ^ bits, jnp.zeros_like(row))]
        return place_blocks(parts, where, (n_row * w_blk.shape[0], w_blk.shape[1]), w_blk.shape[0])

    def scatter_near(make_part):
        row = lax.axis_index('row')
        got_far = flip_row(make_part(row ^ 3), 1)
        got_own = flip_row(make_part(row ^ 1), 1)
        return make_part(row ^ 2) + got_far, got_own

    def scatter_far(make_part, got_own, far):
        return (make_part(lax.axis_index('row')) + got_own + far).astype(BF16)

    def sum_row(val):
        val = val + flip_row(val, 1)
        return val + flip_row(val, 2)

    def layer_block(x_blk, ln1_scale, ln1_shift, w_qkv, b_qkv, w_o, b_o, ln2_scale, ln2_shift, w_in, b_in, w_out, b_out, grad_blk):
        seq_count, seq_len, d_local = x_blk.shape
        tokens = seq_count * seq_len
        heads_local, qkv_width = b_qkv.shape
        head_dim = qkv_width // 3
        width = d_local * n_col
        col = lax.axis_index('col')
        x_rows = x_blk.reshape(tokens, d_local)
        grad_rows = grad_blk.reshape(tokens, d_local)

        def col_block(val, axis, index, size):
            return lax.dynamic_slice_in_dim(val, index * size, size, axis)

        row = lax.axis_index('row')
        near_y = row // 2

        def spread(tok_vals):
            full = jnp.zeros((tokens, d_local), tok_vals.dtype)
            size = tokens // n_col
            for step in range(n_col):
                part = col_block(tok_vals, 1, (col + step) % n_col, d_local)
                part = shift_col(part, step) if step else part
                full = lax.dynamic_update_slice_in_dim(full, part, (col - step) % n_col * size, 0)
            return full

        vec_blk = jnp.stack([ln1_scale, ln1_shift, b_o, ln2_scale, ln2_shift])
        vec_far = [shift_col(vec_blk, step) for step in range(1, n_col)]
        vecs = jnp.zeros((5, width), F32)
        for step, part in enumerate([vec_blk] + vec_far):
            vecs = lax.dynamic_update_slice_in_dim(vecs, part, (col - step) % n_col * d_local, 1)
        s1, t1, bo, s2, t2 = [vecs[i:i + 1] for i in range(5)]

        wo_half = lax.all_gather(half_dp(w_o, 0), 'col', axis=1, tiled=True)
        x_full = lax.all_gather(tie(x_rows, wo_half), 'col', axis=1, tiled=True)
        wq_far = flip_row(w_qkv, 2)
        wo_pair = join_dp(wo_half, 0)
        wi_far = flip_row(tie(w_in, wq_far), 2)
        wi = gather_row(w_in, wi_far)
        wo_far = flip_row(tie(wo_pair, wi_far), 2)
        half_f = w_out.shape[0] // 2
        wq = gather_row(w_qkv, wq_far)
        x_full = tie(x_full, *vec_far)
        w_half = tie(half_dp(w_out, 1), x_full)
        wt_even = cross_even(col_block(w_half, 0, col // 2, half_f))
        wt_odd = cross(col_block(w_half, 0, 1 - col // 2, half_f), lambda r, c: (c ^ 2, r))
        wt_half = jnp.stack(pick(near_y == 0, wt_even, wt_odd))
        x32 = x_full.astype(F32)
        mean1, inv1 = norm_stats(x32, width)
        h1 = ((x32 - mean1) * inv1 * s1 + t1).astype(BF16)
        qkv_dot = dot_nn(h1, wq)
        qkv_rows = (qkv_dot + b_qkv.reshape(heads_local * qkv_width)).astype(BF16)
        attn_rows, attn_stats = attn_forward(qkv_rows, head_dim)
        attn_full = lax.all_gather(attn_rows, 'col', axis=1, tiled=True)

        g_full = lax.all_gather(tie(grad_rows, attn_rows), 'col', axis=1, tiled=True)
        wo = gather_row(wo_pair, wo_far)
        wt_pair = join_dp(wt_half, 2)
        wt_far = flip_row(tie(wt_pair, wo_far), 2)
        attn_full = tie(attn_full, wt_pair)

        r1_dot = dot_nn(attn_full, wo)
        r1 = (x32 + r1_dot + bo).astype(BF16)
        wt_far = tie(wt_far, r1)
        wt_parts = [wt_pair, flip_row(wt_pair, 1), wt_far, flip_row(wt_far, 1)]
        where = [coord for half in (near_y, 1 - near_y) for bit in range(2) for j in range(2) for coord in (half, 2 * j + (row % 2 ^ bit))]
        wt = place_blocks(wt_parts, where, (2 * half_f, width), half_f)
        r32 = r1.astype(F32)
        mean2, inv2 = norm_stats(r32, width)
        h2 = ((r32 - mean2) * inv2 * s2 + t2).astype(BF16)
        pre_act = dot_nn(h2, wi) + b_in
        hidden, gelu_back = jax.vjp(gelu_tanh, pre_act)
        hidden = hidden.astype(BF16)

        out_dot = dot_nn(hidden, wt)
        out_part = lax.psum_scatter(out_dot, 'col', scatter_dimension=1, tiled=True)
        grad_hidden = dot_nt(tie(g_full, out_dot), wt).astype(BF16)
        grad_pre = gelu_back(grad_hidden.astype(F32))[0].astype(BF16)
        tok_local = tokens // n_col
        gn2_dot = dot_nt(grad_pre, wi)
        k_local = width // n_row
        hidden_l, g_l, h2_l, gp_l = lax.optimization_barrier((hidden, g_full, h2, grad_pre, gn2_dot))[:4]

        def wout_part(half, core):
            pair = jnp.concatenate([col_block(g_l, 1, core, d_local), col_block(g_l, 1, 2 + core, d_local)], axis=1)
            return dot_tn(col_block(hidden_l, 1, half, half_f), pair)

        make_win = lambda j: dot_tn(col_block(h2_l, 1, j, k_local), gp_l)
        core = row % 2
        wout_got = flip_row(wout_part(1 - near_y, 1 - core), 1)
        wout_own = flip_row(wout_part(near_y, 1 - core), 1)
        wout_send = wout_part(1 - near_y, core) + wout_got
        wout_far = flip_row(wout_send, 2)
        win_send, win_own = scatter_near(make_win)
        win_far = flip_row(tie(win_send, wout_far), 2)
        gn2 = lax.psum_scatter(tie(gn2_dot, out_part, wout_send, win_send), 'col', scatter_dimension=0, tiled=True)
        wout_sum = (wout_part(near_y, core) + wout_own + wout_far).astype(BF16)
        gn2 = tie(gn2, wout_sum).astype(BF16).astype(F32)
        r_tok = col_block(r1, 0, col, tok_local).astype(F32)
        mean_t, inv_t = col_block(mean2, 0, col, tok_local), col_block(inv2, 0, col, tok_local)
        hat_t = (r_tok - mean_t) * inv_t
        gs2 = jnp.stack([jnp.sum(gn2 * hat_t, axis=0), jnp.sum(gn2, axis=0)])
        ghat = gn2 * s2
        gin = inv_t * (ghat - jnp.mean(ghat, axis=-1, keepdims=True) - hat_t * jnp.mean(ghat * hat_t, axis=-1, keepdims=True))
        gr_tok = (col_block(g_full, 0, col, tok_local).astype(F32) + gin).astype(BF16)
        grad_attn = spread(dot_nt(gr_tok, wo).astype(BF16))
        wout_even = cross_even(col_block(tie(wout_sum, grad_attn), 1, near_y, d_local))
        wout_odd = cross(col_block(tie(wout_sum, grad_attn), 1, 1 - near_y, d_local), lambda r, c: (c, r ^ 2))
        grad_qkv = attn_backward(qkv_rows, grad_attn, attn_stats, head_dim)
        out_rows = (col_block(r1, 1, col, d_local).astype(F32) + out_part + b_out).astype(BF16)

        grad_wout = jnp.concatenate(pick(col // 2 == 0, wout_even, wout_odd), axis=0)
        gn1_dot = dot_nt(grad_qkv, wq)
        gn1 = lax.psum_scatter(gn1_dot, 'col', scatter_dimension=1, tiled=True)
        h1_l, gq_l = lax.optimization_barrier((h1, grad_qkv, gn1_dot))[:2]
        make_wqkv = lambda j: dot_tn(col_block(h1_l, 1, j, k_local), gq_l)
        wqkv_send, wqkv_own = scatter_near(make_wqkv)
        wqkv_far = flip_row(wqkv_send, 2)
        gr_mine = spread(tie(gr_tok, wqkv_send))
        make_wo = lambda j: dot_tn(col_block(attn_full, 1, j, k_local), gr_mine)
        wo_send, wo_own = scatter_near(make_wo)
        gwo_far = flip_row(wo_send, 2)
        grad_wqkv = scatter_far(make_wqkv, wqkv_own, wqkv_far)
        grad_win = scatter_far(make_win, win_own, win_far)
        grad_wo = scatter_far(make_wo, wo_own, gwo_far)
        gn1 = tie(gn1, grad_wqkv, grad_win).astype(BF16).astype(F32)
        hat1 = (x_rows.astype(F32) - mean1) * inv1
        ghat1 = gn1 * ln1_scale
        sums = jnp.stack([jnp.sum(ghat1, axis=-1), jnp.sum(ghat1 * hat1, axis=-1)])
        sums = (sums + shift_col(sums, 1) + shift_col(sums, 2) + shift_col(sums, 3)) / width
        gx = gr_mine.astype(F32) + inv1 * (ghat1 - sums[0][:, None] - hat1 * sums[1][:, None])
        grad_x = gx.astype(BF16)

        def tok_sum(val):
            return jnp.sum(val.astype(F32), axis=0)

        ln2_part = col_block(gs2, 1, col, d_local)
        for step in range(1, n_col):
            ln2_part = ln2_part + shift_col(col_block(gs2, 1, (col + step) % n_col, d_local), step)
        early = sum_row(jnp.concatenate([ln2_part.reshape(-1), tok_sum(grad_rows), tok_sum(gr_mine), tok_sum(grad_pre)]))
        gl2s, gl2t, gbout, gbo, gbin = jnp.split(early, [d_local * k for k in range(1, 5)])
        gbqkv = sum_row(tok_sum(grad_qkv))
        late = sum_row(jnp.stack([jnp.sum(gn1 * hat1, axis=0), jnp.sum(gn1, axis=0)]))
        return (out_rows.reshape(x_blk.shape), grad_x.reshape(x_blk.shape), late[0], late[1], grad_wqkv, gbqkv.reshape(heads_local, qkv_width), grad_wo, gbo, gl2s, gl2t, grad_win, gbin, grad_wout, gbout)

    return jax.shard_map(layer_block, mesh=mesh,
                         in_specs=(act_spec, vec_spec, vec_spec, mat_spec, head_spec, mat_spec, vec_spec, vec_spec, vec_spec, mat_spec, vec_spec, mat_spec, vec_spec, act_spec),
                         out_specs=(act_spec, act_spec, gvec_spec, gvec_spec, gmat_spec, ghead_spec, gmat_spec, gvec_spec, gvec_spec, gvec_spec, gmat_spec, gvec_spec, gmat_spec, gvec_spec),
                         check_vma=False)
```

```python
import functools

import jax
import jax.numpy as jnp
from jax import lax
from jax.experimental import pallas as pl
from jax.experimental.pallas import tpu as pltpu
from jax.sharding import PartitionSpec as P


LN_EPS = 1e-5
BF16 = jnp.bfloat16
F32 = jnp.float32
LOG2E = 1.4426950408889634
MASKED = -1e30


def gelu_tanh(pre_act):
    return jax.nn.gelu(pre_act, approximate=True)


def dot_nn(lhs, rhs):
    return jnp.dot(lhs, rhs, preferred_element_type=F32)


def dot_nt(lhs, rhs):
    return lax.dot_general(lhs, rhs, (((1,), (1,)), ((), ())), preferred_element_type=F32)


def dot_tn(lhs, rhs):
    return lax.dot_general(lhs, rhs, (((0,), (0,)), ((), ())), preferred_element_type=F32)


def split_heads(blk, base, size):
    return blk[:, base:base + size], blk[:, base + size:base + 2 * size], blk[:, base + 2 * size:base + 3 * size]


def causal_mask(step):
    key_pos = lax.broadcasted_iota(jnp.int32, (step, step), 0)
    return key_pos <= lax.broadcasted_iota(jnp.int32, (step, step), 1)


def attn_fwd_kernel(head_dim, step, qkv_ref, out_ref, stat_ref):
    blocks = qkv_ref.shape[0] // step
    factor = head_dim ** -0.5 * LOG2E
    mask = causal_mask(step)
    blk = qkv_ref[...]
    for i in range(blocks):
        rows = slice(i * step, (i + 1) * step)
        outs = []
        for j in range(2):
            query, key, value = split_heads(blk, j * 3 * head_dim, head_dim)
            scores = [dot_nt(key[b * step:(b + 1) * step], query[rows]) for b in range(i + 1)]
            scores[i] = jnp.where(mask, scores[i], MASKED)
            top = functools.reduce(jnp.maximum, [jnp.max(s, axis=0, keepdims=True) for s in scores])
            exps = [jnp.exp2((s - top) * factor) for s in scores]
            inv = 1.0 / sum(jnp.sum(e, axis=0, keepdims=True) for e in exps)
            outs.append(sum(dot_tn(value[b * step:(b + 1) * step], (e * inv).astype(BF16)) for b, e in enumerate(exps)))
            stat_ref[0, 2 * j:2 * j + 1, rows] = top
            stat_ref[0, 2 * j + 1:2 * j + 2, rows] = inv
        out_ref[rows, :] = jnp.concatenate(outs, axis=0).T.astype(BF16)


def attn_bwd_kernel(head_dim, step, qkv_ref, grad_ref, stat_ref, out_ref):
    blocks = qkv_ref.shape[0] // step
    scale = head_dim ** -0.5
    factor = scale * LOG2E
    mask = causal_mask(step)
    blk = qkv_ref[...]
    for j in range(2):
        base = j * 3 * head_dim
        query, key, value = split_heads(blk, base, head_dim)
        grad = grad_ref[:, j * head_dim:(j + 1) * head_dim]
        grad_key, grad_value = [0.0] * blocks, [0.0] * blocks
        for i in range(blocks):
            rows = slice(i * step, (i + 1) * step)
            top = stat_ref[0, 2 * j:2 * j + 1, rows]
            inv = stat_ref[0, 2 * j + 1:2 * j + 2, rows]
            probs, grads, dots = [], [], 0.0
            for b in range(i + 1):
                keys = slice(b * step, (b + 1) * step)
                scores = dot_nt(key[keys], query[rows])
                if b == i:
                    scores = jnp.where(mask, scores, MASKED)
                prob = jnp.exp2((scores - top) * factor) * inv
                grad_prob = dot_nt(value[keys], grad[rows])
                dots = dots + jnp.sum(prob * grad_prob, axis=0, keepdims=True)
                probs.append(prob)
                grads.append(grad_prob)
            grad_query = 0.0
            for b in range(i + 1):
                keys = slice(b * step, (b + 1) * step)
                grad_score = (probs[b] * (grads[b] - dots)).astype(BF16)
                grad_value[b] = grad_value[b] + dot_nn(probs[b].astype(BF16), grad[rows])
                grad_key[b] = grad_key[b] + dot_nn(grad_score, query[rows])
                grad_query = grad_query + dot_tn(key[keys], grad_score)
            out_ref[rows, base:base + head_dim] = (grad_query.T * scale).astype(BF16)
        for b in range(blocks):
            rows = slice(b * step, (b + 1) * step)
            out_ref[rows, base + head_dim:base + 2 * head_dim] = (grad_key[b] * scale).astype(BF16)
            out_ref[rows, base + 2 * head_dim:base + 3 * head_dim] = grad_value[b].astype(BF16)


def attn_cost(tokens, heads, head_dim, dots):
    return pl.CostEstimate(flops=dots * tokens * tokens * heads * head_dim, bytes_accessed=12 * tokens * heads * head_dim, transcendentals=tokens * tokens * heads // 2)


def attn_forward(qkv_rows, head_dim):
    tokens, width = qkv_rows.shape
    pairs = width // (6 * head_dim)
    return pl.pallas_call(
        functools.partial(attn_fwd_kernel, head_dim, 256),
        grid=(pairs,),
        in_specs=[pl.BlockSpec((tokens, 6 * head_dim), lambda p: (0, p))],
        out_specs=[pl.BlockSpec((tokens, 2 * head_dim), lambda p: (0, p)), pl.BlockSpec((1, 8, tokens), lambda p: (p, 0, 0))],
        out_shape=[jax.ShapeDtypeStruct((tokens, 2 * head_dim * pairs), BF16), jax.ShapeDtypeStruct((pairs, 8, tokens), F32)],
        cost_estimate=attn_cost(tokens, 2 * pairs, head_dim, 4),
        name="attn_fwd",
    )(qkv_rows)


def attn_backward(qkv_rows, grad_rows, stats, head_dim):
    tokens, width = qkv_rows.shape
    pairs = width // (6 * head_dim)
    return pl.pallas_call(
        functools.partial(attn_bwd_kernel, head_dim, 256),
        grid=(pairs,),
        in_specs=[pl.BlockSpec((tokens, 6 * head_dim), lambda p: (0, p)), pl.BlockSpec((tokens, 2 * head_dim), lambda p: (0, p)), pl.BlockSpec((1, 8, tokens), lambda p: (p, 0, 0))],
        out_specs=pl.BlockSpec((tokens, 6 * head_dim), lambda p: (0, p)),
        out_shape=jax.ShapeDtypeStruct((tokens, width), BF16),
        cost_estimate=attn_cost(tokens, 2 * pairs, head_dim, 10),
        name="attn_bwd",
    )(qkv_rows, grad_rows, stats)


def place_kernel(count, index_ref, *refs):
    for part in range(count):
        @pl.when(pl.program_id(0) == part)
        def _():
            refs[count][...] = refs[part][0]


def place_blocks(parts, where, shape, tile):
    count = len(parts)
    depth, rows, cols = parts[0].shape
    steps = rows // tile

    def part_map(own):
        def index_map(part, level, step, index_ref):
            active, past = part == own, part > own
            last = jnp.where(past, 1, 0)
            return jnp.where(active, level, last * (depth - 1)), jnp.where(active, step, last * (steps - 1)), 0

        return index_map

    def out_map(part, level, step, index_ref):
        slot = 2 * (part * depth + level)
        return index_ref[slot] * steps + step, index_ref[slot + 1]

    return pl.pallas_call(
        functools.partial(place_kernel, count),
        grid_spec=pltpu.PrefetchScalarGridSpec(
            num_scalar_prefetch=1,
            grid=(count, depth, steps),
            in_specs=[pl.BlockSpec((1, tile, cols), part_map(own)) for own in range(count)],
            out_specs=pl.BlockSpec((tile, cols), out_map),
        ),
        out_shape=jax.ShapeDtypeStruct(shape, parts[0].dtype),
        cost_estimate=pl.CostEstimate(flops=40000000, bytes_accessed=4 * shape[0] * shape[1], transcendentals=0),
        name="place_blocks",
    )(jnp.stack(where).astype(jnp.int32), *parts)


def norm_stats(act_f32, width):
    mean_val = jnp.sum(act_f32, axis=-1, keepdims=True) / width
    mean_sq = jnp.sum(act_f32 * act_f32, axis=-1, keepdims=True) / width
    return mean_val, lax.rsqrt(mean_sq - mean_val * mean_val + LN_EPS)


def solution(mesh):
    n_row, n_col = mesh.shape['row'], mesh.shape['col']
    act_spec = P(('dp', 'row'), None, 'col')
    vec_spec = P('col')
    mat_spec = P('row', 'col')
    head_spec = P('col', None)
    gvec_spec = P(('dp', 'col'))
    gmat_spec = P(('dp', 'row'), 'col')
    ghead_spec = P(('dp', 'col'), None)

    def flip_row(val, bits):
        return lax.ppermute(val, 'row', [(src, src ^ bits) for src in range(n_row)])

    def shift_col(val, step):
        return lax.ppermute(val, 'col', [(src, (src + step) % n_col) for src in range(n_col)])

    def cross(val, route):
        pairs = []
        for r in range(n_row):
            for c in range(n_col):
                row_to, col_to = route(r, c)
                if (row_to, col_to) != (r, c):
                    pairs.append((c * n_row + r, col_to * n_row + row_to))
        return lax.ppermute(val, ('col', 'row'), pairs)

    def cross_even(val):
        moved = cross(val, lambda r, c: (c, r))
        return jnp.where(lax.axis_index('row') == lax.axis_index('col'), val, moved)

    def pick(first, lead, other):
        return jnp.where(first, lead, other), jnp.where(first, other, lead)

    def tie(val, *others):
        return lax.optimization_barrier((val,) + others)[0]

    def swap_dp(val):
        return lax.ppermute(val, 'dp', [(0, 1), (1, 0)])

    def join_dp(half, axis):
        other = swap_dp(half)
        lead = lax.axis_index('dp') == 0
        return jnp.concatenate([jnp.where(lead, half, other), jnp.where(lead, other, half)], axis=axis)

    def half_dp(val, axis):
        size = val.shape[axis] // 2
        return lax.dynamic_slice_in_dim(val, lax.axis_index('dp') * size, size, axis)

    def gather_row(w_blk, far):
        row = lax.axis_index('row')
        mate = flip_row(w_blk, 1)
        far_mate = flip_row(far, 1)
        parts = [part[None] for part in (w_blk, mate, far, far_mate)]
        where = [coord for bits in range(4) for coord in (row ^ bits, jnp.zeros_like(row))]
        return place_blocks(parts, where, (n_row * w_blk.shape[0], w_blk.shape[1]), w_blk.shape[0])

    def scatter_near(make_part):
        row = lax.axis_index('row')
        got_far = flip_row(make_part(row ^ 3), 1)
        got_own = flip_row(make_part(row ^ 1), 1)
        return make_part(row ^ 2) + got_far, got_own

    def scatter_far(make_part, got_own, far):
        return (make_part(lax.axis_index('row')) + got_own + far).astype(BF16)

    def sum_row(val):
        val = val + flip_row(val, 1)
        return val + flip_row(val, 2)

    def layer_block(x_blk, ln1_scale, ln1_shift, w_qkv, b_qkv, w_o, b_o, ln2_scale, ln2_shift, w_in, b_in, w_out, b_out, grad_blk):
        seq_count, seq_len, d_local = x_blk.shape
        tokens = seq_count * seq_len
        heads_local, qkv_width = b_qkv.shape
        head_dim = qkv_width // 3
        width = d_local * n_col
        col = lax.axis_index('col')
        x_rows = x_blk.reshape(tokens, d_local)
        grad_rows = grad_blk.reshape(tokens, d_local)

        def col_block(val, axis, index, size):
            return lax.dynamic_slice_in_dim(val, index * size, size, axis)

        row = lax.axis_index('row')
        near_y = row // 2

        def spread(tok_vals):
            full = jnp.zeros((tokens, d_local), tok_vals.dtype)
            size = tokens // n_col
            for step in range(n_col):
                part = col_block(tok_vals, 1, (col + step) % n_col, d_local)
                part = shift_col(part, step) if step else part
                full = lax.dynamic_update_slice_in_dim(full, part, (col - step) % n_col * size, 0)
            return full

        vec_blk = jnp.stack([ln1_scale, ln1_shift, b_o, ln2_scale, ln2_shift])
        vec_far = [shift_col(vec_blk, step) for step in range(1, n_col)]
        vecs = jnp.zeros((5, width), F32)
        for step, part in enumerate([vec_blk] + vec_far):
            vecs = lax.dynamic_update_slice_in_dim(vecs, part, (col - step) % n_col * d_local, 1)
        s1, t1, bo, s2, t2 = [vecs[i:i + 1] for i in range(5)]

        wo_half = lax.all_gather(half_dp(w_o, 0), 'col', axis=1, tiled=True)
        x_full = lax.all_gather(tie(x_rows, wo_half), 'col', axis=1, tiled=True)
        wq_far = flip_row(w_qkv, 2)
        wo_pair = join_dp(wo_half, 0)
        wi_far = flip_row(tie(w_in, wq_far), 2)
        wi = gather_row(w_in, wi_far)
        wo_far = flip_row(tie(wo_pair, wi_far), 2)
        half_f = w_out.shape[0] // 2
        wq = gather_row(w_qkv, wq_far)
        x_full = tie(x_full, *vec_far)
        w_half = tie(half_dp(w_out, 1), x_full)
        wt_even = cross_even(col_block(w_half, 0, col // 2, half_f))
        wt_odd = cross(col_block(w_half, 0, 1 - col // 2, half_f), lambda r, c: (c ^ 2, r))
        wt_half = jnp.stack(pick(near_y == 0, wt_even, wt_odd))
        x32 = x_full.astype(F32)
        mean1, inv1 = norm_stats(x32, width)
        h1 = ((x32 - mean1) * inv1 * s1 + t1).astype(BF16)
        qkv_dot = dot_nn(h1, wq)
        qkv_rows = (qkv_dot + b_qkv.reshape(heads_local * qkv_width)).astype(BF16)
        attn_rows, attn_stats = attn_forward(qkv_rows, head_dim)
        attn_full = lax.all_gather(attn_rows, 'col', axis=1, tiled=True)

        g_full = lax.all_gather(tie(grad_rows, attn_rows), 'col', axis=1, tiled=True)
        wo = gather_row(wo_pair, wo_far)
        wt_pair = join_dp(wt_half, 2)
        wt_far = flip_row(tie(wt_pair, wo_far), 2)
        attn_full = tie(attn_full, wt_pair)

        r1_dot = dot_nn(attn_full, wo)
        r1 = (x32 + r1_dot + bo).astype(BF16)
        wt_far = tie(wt_far, r1)
        wt_parts = [wt_pair, flip_row(wt_pair, 1), wt_far, flip_row(wt_far, 1)]
        where = [coord for half in (near_y, 1 - near_y) for bit in range(2) for j in range(2) for coord in (half, 2 * j + (row % 2 ^ bit))]
        wt = place_blocks(wt_parts, where, (2 * half_f, width), half_f)
        r32 = r1.astype(F32)
        mean2, inv2 = norm_stats(r32, width)
        h2 = ((r32 - mean2) * inv2 * s2 + t2).astype(BF16)
        pre_act = dot_nn(h2, wi) + b_in
        hidden, gelu_back = jax.vjp(gelu_tanh, pre_act)
        hidden = hidden.astype(BF16)

        out_dot = dot_nn(hidden, wt)
        out_part = lax.psum_scatter(out_dot, 'col', scatter_dimension=1, tiled=True)
        grad_hidden = dot_nt(tie(g_full, out_dot), wt).astype(BF16)
        grad_pre = gelu_back(grad_hidden.astype(F32))[0].astype(BF16)
        tok_local = tokens // n_col
        gn2_dot = dot_nt(grad_pre, wi)
        k_local = width // n_row
        hidden_l, g_l, h2_l, gp_l = lax.optimization_barrier((hidden, g_full, h2, grad_pre, gn2_dot))[:4]

        def wout_part(half, core):
            pair = jnp.concatenate([col_block(g_l, 1, core, d_local), col_block(g_l, 1, 2 + core, d_local)], axis=1)
            return dot_tn(col_block(hidden_l, 1, half, half_f), pair)

        make_win = lambda j: dot_tn(col_block(h2_l, 1, j, k_local), gp_l)
        core = row % 2
        wout_got = flip_row(wout_part(1 - near_y, 1 - core), 1)
        wout_own = flip_row(wout_part(near_y, 1 - core), 1)
        wout_send = wout_part(1 - near_y, core) + wout_got
        wout_far = flip_row(wout_send, 2)
        win_send, win_own = scatter_near(make_win)
        win_far = flip_row(tie(win_send, wout_far), 2)
        gn2 = lax.psum_scatter(tie(gn2_dot, out_part, wout_send, win_send), 'col', scatter_dimension=0, tiled=True)
        wout_sum = (wout_part(near_y, core) + wout_own + wout_far).astype(BF16)
        gn2 = tie(gn2, wout_sum).astype(BF16).astype(F32)
        r_tok = col_block(r1, 0, col, tok_local).astype(F32)
        mean_t, inv_t = col_block(mean2, 0, col, tok_local), col_block(inv2, 0, col, tok_local)
        hat_t = (r_tok - mean_t) * inv_t
        gs2 = jnp.stack([jnp.sum(gn2 * hat_t, axis=0), jnp.sum(gn2, axis=0)])
        ghat = gn2 * s2
        gin = inv_t * (ghat - jnp.mean(ghat, axis=-1, keepdims=True) - hat_t * jnp.mean(ghat * hat_t, axis=-1, keepdims=True))
        gr_tok = (col_block(g_full, 0, col, tok_local).astype(F32) + gin).astype(BF16)
        grad_attn = spread(dot_nt(gr_tok, wo).astype(BF16))
        gr_mine = spread(tie(gr_tok, grad_attn))
        wout_even = cross_even(col_block(tie(wout_sum, grad_attn), 1, near_y, d_local))
        wout_odd = cross(col_block(tie(wout_sum, grad_attn), 1, 1 - near_y, d_local), lambda r, c: (c, r ^ 2))
        grad_qkv = attn_backward(qkv_rows, grad_attn, attn_stats, head_dim)
        out_rows = (col_block(r1, 1, col, d_local).astype(F32) + out_part + b_out).astype(BF16)

        grad_wout = jnp.concatenate(pick(col // 2 == 0, wout_even, wout_odd), axis=0)
        gn1_dot = dot_nt(grad_qkv, wq)
        gn1 = lax.psum_scatter(gn1_dot, 'col', scatter_dimension=1, tiled=True)
        h1_l, gq_l = lax.optimization_barrier((h1, grad_qkv, gn1_dot))[:2]
        make_wqkv = lambda j: dot_tn(col_block(h1_l, 1, j, k_local), gq_l)
        wqkv_send, wqkv_own = scatter_near(make_wqkv)
        wqkv_far = flip_row(wqkv_send, 2)
        gr_l = tie(gr_mine, wqkv_send)
        make_wo = lambda j: dot_tn(col_block(attn_full, 1, j, k_local), gr_l)
        wo_send, wo_own = scatter_near(make_wo)
        gwo_far = flip_row(wo_send, 2)
        grad_wqkv = scatter_far(make_wqkv, wqkv_own, wqkv_far)
        grad_win = scatter_far(make_win, win_own, win_far)
        grad_wo = scatter_far(make_wo, wo_own, gwo_far)
        gs2 = tie(gs2, gn1)
        gn1_raw = gn1
        gn1 = tie(gn1, grad_win).astype(BF16).astype(F32)
        hat1 = (x_rows.astype(F32) - mean1) * inv1
        ghat1 = gn1 * ln1_scale
        sums = jnp.stack([jnp.sum(ghat1, axis=-1), jnp.sum(ghat1 * hat1, axis=-1)])
        sums = (sums + shift_col(sums, 1) + shift_col(sums, 2) + shift_col(sums, 3)) / width
        gx = gr_mine.astype(F32) + inv1 * (ghat1 - sums[0][:, None] - hat1 * sums[1][:, None])
        grad_x = gx.astype(BF16)

        def tok_sum(val):
            return jnp.sum(val.astype(F32), axis=0)

        ln2_part = col_block(gs2, 1, col, d_local)
        for step in range(1, n_col):
            ln2_part = ln2_part + shift_col(col_block(gs2, 1, (col + step) % n_col, d_local), step)
        sums_early = tie(jnp.concatenate([tok_sum(grad_rows), tok_sum(gr_mine), tok_sum(grad_pre), tok_sum(grad_qkv)]), gn1_raw)
        small = sum_row(jnp.concatenate([ln2_part.reshape(-1), jnp.sum(gn1 * hat1, axis=0), jnp.sum(gn1, axis=0), sums_early]))
        gl2s, gl2t, gl1s, gl1t, gbout, gbo, gbin, gbqkv = jnp.split(small, [d_local * k for k in (1, 2, 3, 4, 5, 6, 6 + n_col)])
        return (out_rows.reshape(x_blk.shape), grad_x.reshape(x_blk.shape), gl1s, gl1t, grad_wqkv, gbqkv.reshape(heads_local, qkv_width), grad_wo, gbo, gl2s, gl2t, grad_win, gbin, grad_wout, gbout)

    return jax.shard_map(layer_block, mesh=mesh,
                         in_specs=(act_spec, vec_spec, vec_spec, mat_spec, head_spec, mat_spec, vec_spec, vec_spec, vec_spec, mat_spec, vec_spec, mat_spec, vec_spec, act_spec),
                         out_specs=(act_spec, act_spec, gvec_spec, gvec_spec, gmat_spec, ghead_spec, gmat_spec, gvec_spec, gvec_spec, gvec_spec, gmat_spec, gvec_spec, gmat_spec, gvec_spec),
                         check_vma=False)
```
